32 devices in a mesh: dp: 4 (over y, x), vocab: 8 (over z, core).
Axes of the slice: x: 2, y: 2, z: 4, core: 2. Of those that a mesh axis runs over, the one named last changes fastest.
Arguments:
- token_ids: int32 [131072], P(('dp', 'vocab')), may hold values from 0 to 7679, as said below
- valid_counts: int32 [1024], P(('dp', 'vocab')), may hold values from 64 to 128
- grad_output: bfloat16 [131072, 768], P(('dp', 'vocab')), may hold values from -6 to 6
- pre_norm: bfloat16 [131072, 768], P(('dp', 'vocab')), may hold values from -6 to 6
- norm_gain: float32 [768], replicated, may hold values from 0.5 to 1.5
Outputs:
- grad_table: float32 [7680, 768], P('vocab')
The draws below stay inside these ranges and needn't reach their ends.
Inputs may be any that keep to these rules, and one draw needn't show every extreme that they name: `token_ids`: of the 4096 positions of one device, at most 1024 have ids in any one range [k * 960, (k + 1) * 960); in every group of 8 consecutive devices one such range takes exactly 1024 from every device of the group. Padding positions carry ids too.
All inputs are finite; a program needn't handle non-finite values.
Results may differ from the reference program's by a relative error of at most 0.0029.
Values may be sent and summed in bfloat16 or wider, within the bound.
No kernel may reach another device: no remote copies, remote signals or barrier semaphores. Data moves between devices by JAX's collectives and lax.ppermute only.
A program may use at most 128 MiB of HBM per device.

```python
import jax
import jax.numpy as jnp
from jax import lax

D = 768
VOCAB_DEV = 960
BLOCK = 128
TOK_DEV = 4096
VOCAB = 7680
TOKENS = 131072
BLOCKS = 1024
CAP = 1024
N_DP = 4
N_VOCAB = 8
DEVICES = 32


def draw_token_ids(key, part):
    keys = jax.random.split(key, 6)
    slots = N_VOCAB * CAP
    hottest = jax.random.randint(keys[0], (N_DP,), 0, N_VOCAB)
    hot_dev = jnp.repeat(hottest, N_VOCAB)
    prefer = jax.random.randint(keys[1], (DEVICES, N_VOCAB), 0, 4)
    noise = jax.random.randint(keys[2], (DEVICES, slots), 0, 4096)
    owner_of = jnp.arange(slots, dtype=jnp.int32) // CAP
    score = prefer[:, owner_of] * 4096 + noise
    score = jnp.where(owner_of[None, :] == hot_dev[:, None], -1, score)
    score = score * slots + jnp.arange(slots, dtype=jnp.int32)[None, :]
    chosen = jnp.argsort(score, axis=1, stable=True)[:, :TOK_DEV]
    owners = chosen // CAP
    owners = jax.random.permutation(keys[3], owners, axis=1, independent=True)
    first_term = jax.random.randint(keys[4], (DEVICES, TOK_DEV), 0, VOCAB_DEV)
    second_term = jax.random.randint(keys[5], (DEVICES, TOK_DEV), 0, VOCAB_DEV)
    offsets = jnp.minimum(first_term, second_term)
    return (owners * VOCAB_DEV + offsets).reshape(-1).astype(jnp.int32)


def plant(entries, stream_key, low, top_value):
    spot = [jax.random.randint(jax.random.fold_in(stream_key, axis), (), 0, length) for axis, length in enumerate(entries.shape)]
    widest = entries.shape.index(max(entries.shape))
    next_to = spot[:widest] + [(spot[widest] + 1) % entries.shape[widest]] + spot[widest + 1:]
    return entries.at[tuple(spot)].set(low).at[tuple(next_to)].set(top_value)


def steps_of(key, dims, cuts, smallest, high):
    level = 1.0
    for axis_at, blocks in cuts:
        draws = jax.random.uniform(jax.random.fold_in(jax.random.fold_in(key, 6), axis_at), (blocks,), jnp.float32, smallest / len(cuts), high / len(cuts))
        level = level * jnp.repeat(jnp.exp(draws), dims[axis_at] // blocks).reshape((-1,) + (1,) * (len(dims) - 1 - axis_at))
    return level


def normal_values(rng, dims, deviation, bound, shards=(), held_as=jnp.bfloat16):
    array = deviation * jax.random.normal(rng, dims, jnp.float32)
    if shards:
        array = array * steps_of(rng, dims, shards, -0.22, 0.18)
    return jnp.clip(array, -bound, bound).astype(held_as)


def setup_inputs(seed: int = 0) -> dict:
    arg_keys = jax.random.split(jax.random.key(seed), 6)
    return {
        "token_ids": draw_token_ids(jax.random.fold_in(arg_keys[5], 71), 0),
        "valid_counts": plant(jax.random.randint(arg_keys[1], (BLOCKS,), 64, BLOCK + 1), jax.random.fold_in(arg_keys[1], 1), 64, BLOCK).astype(jnp.int32),
        "grad_output": normal_values(arg_keys[2], (TOKENS, D), 1.0, 6.0, ((0, 32),)),
        "pre_norm": normal_values(arg_keys[3], (TOKENS, D), 1.0, 6.0, ((0, 32),)),
        "norm_gain": jnp.clip(1.0 + 0.1 * jax.random.normal(arg_keys[4], (D,), jnp.float32), 0.5, 1.5),
    }


def row_grads(grads, values, counts, gain):
    x = values.astype(jnp.float32)
    mu = lax.optimization_barrier(jnp.mean(x, axis=1, keepdims=True))
    centered_input = x - mu
    inverse_deviation = lax.rsqrt(lax.optimization_barrier(jnp.mean(centered_input * centered_input, axis=1, keepdims=True)) + 1e-12)
    normalized_input = centered_input * inverse_deviation
    scaled_gradient = gain[None, :] * grads.astype(jnp.float32)
    first_term = lax.optimization_barrier(jnp.mean(scaled_gradient, axis=1, keepdims=True))
    second_term = lax.optimization_barrier(jnp.mean(scaled_gradient * normalized_input, axis=1, keepdims=True))
    input_gradient = inverse_deviation * (scaled_gradient - first_term - normalized_input * second_term)
    place = jnp.arange(x.shape[0], dtype=jnp.int32) % BLOCK
    alive = place < jnp.repeat(counts, BLOCK)
    return jnp.where(alive[:, None], input_gradient, 0.0).astype(jnp.bfloat16)

def reference(token_ids, valid_counts, grad_output, pre_norm, norm_gain):
    ids = token_ids.reshape(DEVICES, TOK_DEV)
    counts = valid_counts.reshape(DEVICES, TOK_DEV // BLOCK)
    grads = grad_output.reshape(DEVICES, TOK_DEV, D)
    values = pre_norm.reshape(DEVICES, TOK_DEV, D)

    def step(table, item):
        ids_part, count_part, grad_part, value_part = item
        rows = row_grads(grad_part, value_part, count_part, norm_gain)
        table = table + jax.ops.segment_sum(rows.astype(jnp.float32), ids_part, num_segments=VOCAB)
        return (table, None)
    start = jnp.zeros((VOCAB, D), jnp.float32)
    table, _ = lax.scan(step, start, (ids, counts, grads, values))
    return table
```

```python
import functools

import jax
import jax.numpy as jnp
from jax import lax
from jax.experimental import pallas as pl
from jax.experimental.pallas import tpu as pltpu
from jax.sharding import PartitionSpec as P

VOCAB_DEV = 960
BLOCK = 128


def ln_kernel(counts, g_ref, x_ref, gain_ref, o_ref):
    step = pl.program_id(0)
    per = g_ref.shape[0] // BLOCK
    width = g_ref.shape[1]
    gain = gain_ref[...]
    place = lax.broadcasted_iota(jnp.int32, (BLOCK, 1), 0)
    for b in range(per):
        rows = pl.ds(b * BLOCK, BLOCK)
        x = x_ref[rows, :].astype(jnp.float32)
        mu = jnp.sum(x, axis=1, keepdims=True) * (1.0 / width)
        cen = x - mu
        var = jnp.sum(cen * cen, axis=1, keepdims=True) * (1.0 / width)
        inv = lax.rsqrt(var + 1e-12)
        sg = gain * g_ref[rows, :].astype(jnp.float32)
        m1 = jnp.sum(sg, axis=1, keepdims=True) * (1.0 / width)
        m2 = jnp.sum(sg * cen, axis=1, keepdims=True) * (1.0 / width) * inv
        keep = jnp.where(place < counts[step * per + b], inv, 0.0)
        o_ref[rows, :] = (keep * (sg - m1 - cen * (inv * m2))).astype(jnp.bfloat16)


def row_grads(grads, values, counts, gain):
    toks, width = grads.shape
    tile = 512
    return pl.pallas_call(
        ln_kernel,
        out_shape=jax.ShapeDtypeStruct((toks, width), jnp.bfloat16),
        grid_spec=pltpu.PrefetchScalarGridSpec(
            num_scalar_prefetch=1,
            grid=(toks // tile,),
            in_specs=[
                pl.BlockSpec((tile, width), lambda i, c: (i, 0)),
                pl.BlockSpec((tile, width), lambda i, c: (i, 0)),
                pl.BlockSpec((1, width), lambda i, c: (0, 0)),
            ],
            out_specs=pl.BlockSpec((tile, width), lambda i, c: (i, 0)),
        ),
        compiler_params=pltpu.CompilerParams(vmem_limit_bytes=32 << 20),
        name="ln_grad",
    )(counts, grads, values, gain.reshape(1, width))


def table_kernel(n_seg, seg_rows, shards, starts, ids_a, ids_b, dx_a, dx_b, *outs):
    base = shards[pl.program_id(0)] * VOCAB_DEV
    toks = dx_a.shape[0]
    chunk = 512
    acc = None
    iota = lax.broadcasted_iota(jnp.int32, (seg_rows, 1), 0)
    want = jnp.concatenate([iota + (base + starts[s]) for s in range(n_seg)], axis=0)
    for ids, dx in ((ids_a, dx_a), (ids_b, dx_b)):
        for k in range(toks // chunk):
            cols = pl.ds(k * chunk, chunk)
            pick = jnp.where(want == ids[:, cols], 1.0, 0.0).astype(jnp.bfloat16)
            part = jnp.dot(pick, dx[cols, :], preferred_element_type=jnp.float32)
            acc = part if acc is None else acc + part
    for s in range(n_seg):
        outs[s][0] = acc[s * seg_rows : (s + 1) * seg_rows].astype(outs[s].dtype)


def table_parts(ids_a, ids_b, dx_a, dx_b, shards, starts, seg_rows, dtype, name):
    toks, width = dx_a.shape
    n_seg = starts.shape[0]
    count = shards.shape[0]
    whole = lambda i, a, b: (0, 0)
    return pl.pallas_call(
        functools.partial(table_kernel, n_seg, seg_rows),
        out_shape=[jax.ShapeDtypeStruct((count, seg_rows, width), dtype)] * n_seg,
        grid_spec=pltpu.PrefetchScalarGridSpec(
            num_scalar_prefetch=2,
            grid=(count,),
            in_specs=[
                pl.BlockSpec((1, toks), whole),
                pl.BlockSpec((1, toks), whole),
                pl.BlockSpec((toks, width), whole),
                pl.BlockSpec((toks, width), whole),
            ],
            out_specs=[pl.BlockSpec((1, seg_rows, width), lambda i, a, b: (i, 0, 0))] * n_seg,
        ),
        compiler_params=pltpu.CompilerParams(vmem_limit_bytes=56 << 20),
        name=name,
    )(shards, starts, ids_a, ids_b, dx_a, dx_b)


def per_device(token_ids, valid_counts, grad_output, pre_norm, norm_gain):
    toks = token_ids.shape[0]
    width = grad_output.shape[1]
    n_vocab = lax.axis_size("vocab")
    n_dp = lax.axis_size("dp")
    groups = n_vocab // 2
    half = VOCAB_DEV // 5
    quarter = half // 2
    me = lax.axis_index("vocab")
    core = me % 2
    grp = me // 2
    d = lax.axis_index("dp")
    bx = d % 2
    by = d // 2

    def hop(a, axis, mask):
        n = n_vocab if axis == "vocab" else n_dp
        return lax.ppermute(a, axis, [(i, i ^ mask) for i in range(n)])

    ids_a = token_ids.reshape(1, toks)
    ids_b = hop(ids_a, "vocab", 1)
    dx_a = row_grads(grad_output, pre_norm, valid_counts, norm_gain)
    dx_b = hop(dx_a, "vocab", 1)
    base1 = 0
    base2 = 2 * half
    base3 = 4 * half
    every = 2 * jnp.arange(groups, dtype=jnp.int32) + core
    others = 2 * (jnp.arange(1, groups, dtype=jnp.int32) ^ grp) + core
    vec = lambda *v: jnp.stack([jnp.asarray(i, jnp.int32) for i in v])
    build = functools.partial(table_parts, ids_a, ids_b, dx_a, dx_b)
    send_x, send_y = build(
        every,
        vec(base1 + (1 - bx) * half, base2 + (1 - by) * half),
        half, jnp.bfloat16, "send_xy",
    )
    (send_z,) = build(others, vec(base3), half, jnp.bfloat16, "send_z")
    got_x = hop(send_x, "dp", 1)
    got_y = hop(send_y, "dp", 2)
    got_z = [hop(send_z[k - 1], "vocab", 2 * k) for k in range(1, groups)]
    own_x, own_y = build(
        every,
        vec(base1 + bx * half, base2 + by * half),
        half, jnp.float32, "own_xy",
    )
    (own_z,) = build(vec(me), vec(base3), half, jnp.float32, "own_z")

    def split(own, got, bit):
        mine = lax.dynamic_slice_in_dim(own, bit * quarter, quarter, 1) + lax.dynamic_slice_in_dim(
            got, bit * quarter, quarter, 1
        ).astype(jnp.float32)
        give = lax.dynamic_slice_in_dim(own, (1 - bit) * quarter, quarter, 1) + lax.dynamic_slice_in_dim(
            got, (1 - bit) * quarter, quarter, 1
        ).astype(jnp.float32)
        return mine, give.astype(jnp.bfloat16)

    mine1, give1 = split(own_x, got_x, by)
    mine2, give2 = split(own_y, got_y, bx)
    got1 = hop(give1, "dp", 2)
    got2 = hop(give2, "dp", 1)
    q1 = mine1 + got1.astype(jnp.float32)
    q2 = mine2 + got2.astype(jnp.float32)
    q = jnp.concatenate([q1, q2], axis=1)
    q_send = q.astype(jnp.bfloat16)
    fin = lax.dynamic_index_in_dim(q, grp, 0, keepdims=False)
    for k in range(1, groups):
        piece = lax.dynamic_index_in_dim(q_send, grp ^ k, 0, keepdims=False)
        fin = fin + hop(piece, "vocab", 2 * k).astype(jnp.float32)
    fin = fin.astype(jnp.bfloat16)

    sum_z = own_z[0]
    for piece in got_z:
        sum_z = sum_z + piece.astype(jnp.float32)
    za, zb = sum_z[:quarter].astype(jnp.bfloat16), sum_z[quarter:].astype(jnp.bfloat16)
    za = (za.astype(jnp.float32) + hop(za, "dp", 1).astype(jnp.float32)).astype(jnp.bfloat16)
    zb = (zb.astype(jnp.float32) + hop(zb, "dp", 2).astype(jnp.float32)).astype(jnp.bfloat16)
    za = za.astype(jnp.float32) + hop(za, "dp", 2).astype(jnp.float32)
    zb = zb.astype(jnp.float32) + hop(zb, "dp", 1).astype(jnp.float32)

    s1, s2 = fin[:quarter], fin[quarter:]
    t1 = hop(s1, "dp", 2)
    t2 = hop(s2, "dp", 1)

    def pair(a, b, bit):
        return jnp.where(bit == 0, jnp.concatenate([a, b], 0), jnp.concatenate([b, a], 0))

    h1 = pair(s1, t1, by)
    h2 = pair(s2, t2, bx)
    u1 = hop(h1, "dp", 1)
    u2 = hop(h2, "dp", 2)
    w1 = pair(h1, u1, bx)
    w2 = pair(h2, u2, by)
    return jnp.concatenate(
        [w1.astype(jnp.float32), w2.astype(jnp.float32), za, zb], axis=0
    )


def solution(mesh):
    in_specs = (
        P(("dp", "vocab")),
        P(("dp", "vocab")),
        P(("dp", "vocab"), None),
        P(("dp", "vocab"), None),
        P(),
    )
    return jax.shard_map(
        per_device, mesh=mesh, in_specs=in_specs, out_specs=P("vocab", None), check_vma=False
    )
```
